128 devices in a mesh: gossip: 32 (over z, y_lo, x), mp: 4 (over y_hi, core).
Axes of the slice: x: 4, y: 4 (y_hi: 2, y_lo: 2; y = y_hi * 2 + y_lo), z: 4, core: 2. Of those that a mesh axis runs over, the one named last changes fastest.
Arguments:
- tokens: bfloat16 [32, 512, 2048], P('gossip'), may hold values from -6 to 6
- targets: bfloat16 [32, 512, 2048], P('gossip'), may hold values from -6 to 6
- gate_weight: bfloat16 [32, 2048, 4096], P('gossip', None, 'mp'), may hold values from -6 to 6
- up_weight: bfloat16 [32, 2048, 4096], P('gossip', None, 'mp'), may hold values from -6 to 6
- down_weight: bfloat16 [32, 4096, 2048], P('gossip', 'mp'), may hold values from -6 to 6
Outputs:
- gate_out: bfloat16 [32, 2048, 4096], P('gossip', None, 'mp')
- up_out: bfloat16 [32, 2048, 4096], P('gossip', None, 'mp')
- down_out: bfloat16 [32, 4096, 2048], P('gossip', 'mp')
The draws below stay inside these ranges and needn't reach their ends.
All inputs are finite; a program needn't handle non-finite values.
Results may differ from the reference program's by a relative error of at most 0.0095.
Values may be sent and summed in bfloat16 or wider, within the bound.
No kernel may reach another device: no remote copies, remote signals or barrier semaphores. Data moves between devices by JAX's collectives and lax.ppermute only.
A program may use at most 128 MiB of HBM per device.

```python
import jax
import jax.numpy as jnp
from jax import lax

D = 2048
TOK = 512
ITERS = 1
FF = 4096
REPLICAS = 32


def levels(own_key, dims, pieces, least, largest):
    gain = 1.0
    for dim, blocks in pieces:
        steps = jax.random.uniform(jax.random.fold_in(jax.random.fold_in(own_key, 6), dim), (blocks,), jnp.float32, least / len(pieces), largest / len(pieces))
        gain = gain * jnp.repeat(jnp.exp(steps), dims[dim] // blocks).reshape((-1,) + (1,) * (len(dims) - 1 - dim))
    return gain


def bell_draw(stream_key, extent, spread, reach, split=(), kind=jnp.bfloat16):
    values = spread * jax.random.normal(stream_key, extent, jnp.float32)
    if split:
        values = values * levels(stream_key, extent, split, -0.22, 0.18)
    return jnp.clip(values, -reach, reach).astype(kind)


def setup_inputs(seed: int = 0) -> dict:
    keys = jax.random.split(jax.random.key(seed), 6)
    return {
        "tokens": bell_draw(keys[0], (REPLICAS, TOK, D), 1.0, 6.0, ((0, 32),)),
        "targets": bell_draw(keys[1], (REPLICAS, TOK, D), 1.0, 6.0, ((0, 32),)),
        "gate_weight": bell_draw(keys[2], (REPLICAS, D, FF), 1.0, 6.0, ((0, 32), (2, 4))),
        "up_weight": bell_draw(keys[3], (REPLICAS, D, FF), 1.0, 6.0, ((0, 32), (2, 4))),
        "down_weight": bell_draw(keys[4], (REPLICAS, FF, D), 1.0, 6.0, ((0, 32), (1, 4))),
    }


def rms_norm(values):
    widened = values.astype(jnp.float32)
    return (widened * lax.rsqrt(lax.optimization_barrier(jnp.mean(widened * widened, axis=-1, keepdims=True)) + 1e-06)).astype(jnp.bfloat16)

def mix_cycle(stepped):
    widened = stepped.astype(jnp.float32)
    total = jnp.roll(widened, 1, axis=0) + widened + jnp.roll(widened, -1, axis=0)
    return (total / 3.0).astype(jnp.bfloat16)

def reference(tokens, targets, gate_weight, up_weight, down_weight):
    tok_count = tokens.shape[1]
    width = tokens.shape[2]
    hidden_all = gate_weight.shape[2]
    in_scale = 1.0 / width ** 0.5
    mid_scale = 1.0 / hidden_all ** 0.5
    step_size = hidden_all / 4.0
    normed = rms_norm(tokens).astype(jnp.float32)
    offset = tokens.astype(jnp.float32) - targets.astype(jnp.float32)
    w_gate, w_up, w_down = (gate_weight, up_weight, down_weight)
    for iteration in range(ITERS):
        gate_pre = jnp.einsum('rtd,rdf->rtf', normed, w_gate.astype(jnp.float32)) * in_scale
        up_pre = jnp.einsum('rtd,rdf->rtf', normed, w_up.astype(jnp.float32)) * in_scale
        sig_gate = jax.nn.sigmoid(gate_pre)
        act_gate = gate_pre * sig_gate
        hidden = (act_gate * up_pre).astype(jnp.bfloat16).astype(jnp.float32)
        output = jnp.einsum('rtf,rfd->rtd', hidden, w_down.astype(jnp.float32)) * mid_scale
        err_grad = ((offset + output) / tok_count).astype(jnp.bfloat16).astype(jnp.float32)
        grad_down = jnp.einsum('rtf,rtd->rfd', hidden, err_grad) * mid_scale
        grad_hidden = jnp.einsum('rtd,rfd->rtf', err_grad, w_down.astype(jnp.float32)) * mid_scale
        grad_gate = (grad_hidden * up_pre * (sig_gate * (1.0 + gate_pre * (1.0 - sig_gate)))).astype(jnp.bfloat16).astype(jnp.float32)
        grad_up = (grad_hidden * act_gate).astype(jnp.bfloat16).astype(jnp.float32)
        grad_wgate = jnp.einsum('rtd,rtf->rdf', normed, grad_gate) * in_scale
        grad_wup = jnp.einsum('rtd,rtf->rdf', normed, grad_up) * in_scale
        new_gate = (w_gate.astype(jnp.float32) - step_size * grad_wgate).astype(jnp.bfloat16)
        new_up = (w_up.astype(jnp.float32) - step_size * grad_wup).astype(jnp.bfloat16)
        new_down = (w_down.astype(jnp.float32) - step_size * grad_down).astype(jnp.bfloat16)
        w_gate = mix_cycle(new_gate)
        w_up = mix_cycle(new_up)
        w_down = mix_cycle(new_down)
    return (w_gate, w_up, w_down)
```

```python
import jax
import jax.numpy as jnp
from jax import lax
from jax.experimental import pallas as pl
from jax.experimental.pallas import tpu as pltpu
from jax.sharding import PartitionSpec as P


SIZES = (256, 256, 512)
UP_ROWS = (1536, 256, 128, 128)
BLOCK = 256
MIB = 1024 * 1024


def along_cycle(value, steps):
    count = lax.axis_size("gossip")
    return lax.ppermute(value, "gossip", [(s, (s + steps) % count) for s in range(count)])


def other_core(value):
    count = lax.axis_size("mp")
    return lax.ppermute(value, "mp", [(s, s ^ 1) for s in range(count)])


def other_chip(value):
    count = lax.axis_size("mp")
    return lax.ppermute(value, "mp", [(s, s ^ 2) for s in range(count)])


def both_ways(value):
    lower = along_cycle(value, 1)
    upper = along_cycle(value, -1)
    return lower, value, upper


def mix_three(lower, own, upper):
    total = lower.astype(jnp.float32) + own.astype(jnp.float32) + upper.astype(jnp.float32)
    return (total / 3.0).astype(jnp.bfloat16)


def mix_rows(before, rows_out, start, parts):
    rows, width = parts[1].shape
    block = min(rows, 256)

    def body(lower, own, upper, *rest):
        rest[-1][...] = mix_three(lower[...], own[...], upper[...])

    piece = pl.BlockSpec((block, width), lambda n: (n, 0))
    aliased = before is not None and before.shape[0] == rows_out
    extra = [] if before is None else [before]
    return pl.pallas_call(
        body,
        grid=(rows // block,),
        in_specs=[piece] * 3 + [pl.BlockSpec(memory_space=pl.ANY)] * len(extra),
        out_specs=pl.BlockSpec((block, width), lambda n: (start // block + n, 0)),
        out_shape=jax.ShapeDtypeStruct((rows_out, width), jnp.bfloat16),
        input_output_aliases={3: 0} if start else {},
        compiler_params=pltpu.CompilerParams(vmem_limit_bytes=56 * MIB),
    )(*parts, *extra)


def dot(a, b, dims):
    return lax.dot_general(a, b, (dims, ((), ())), preferred_element_type=jnp.float32)


def forward_body(core, *refs, in_scale):
    count = len(SIZES)
    tokens, targets, w_gate, w_up, w_down = refs[:5]
    outs = refs[5 : 9 + 3 * count]
    (
        tok, gate_v, up_v, down_t, down_m, wanted,
        hidden, hidden_t, slope, act, normed, theirs, mine, offset, in_sems, out_sems,
    ) = refs[9 + 3 * count :]
    rows, width = tok.shape
    half = width // 2
    blocks = hidden.shape[1] // BLOCK
    at_mine = pl.multiple_of(core[0] * half, half)
    at_theirs = pl.multiple_of((1 - core[0]) * half, half)

    def fetch(n, src, dst):
        return pltpu.make_async_copy(src, dst, in_sems.at[n])

    def put(n, src, dst):
        copy = pltpu.make_async_copy(src, dst, out_sems.at[n])
        copy.start()
        return copy

    def span(n):
        return slice(n * BLOCK, (n + 1) * BLOCK)

    tok_copies = [
        fetch(n, tokens.at[part], tok.at[part])
        for n, part in enumerate((slice(0, rows // 2), slice(rows // 2, rows)))
    ]
    weight_copies = [
        (
            fetch(2 + 2 * n, w_gate.at[:, span(n)], gate_v.at[:, span(n)]),
            fetch(3 + 2 * n, w_up.at[:, span(n)], up_v.at[:, span(n)]),
        )
        for n in range(blocks)
    ]
    base = 2 + 2 * blocks
    copy_t = fetch(base, w_down.at[:, pl.ds(at_theirs, half)], down_t)
    copy_m = fetch(base + 1, w_down.at[:, pl.ds(at_mine, half)], down_m)
    copy_w = fetch(base + 2, targets.at[:, pl.ds(at_mine, half)], wanted)

    for copy in (*tok_copies, *weight_copies[0]):
        copy.start()
    for n, copy in enumerate(tok_copies):
        copy.wait()
        part = slice(n * (rows // 2), (n + 1) * (rows // 2))
        wide = tok[part].astype(jnp.float32)
        scale = lax.rsqrt(jnp.mean(wide * wide, axis=-1, keepdims=True) + 1e-06)
        normed[part] = (wide * scale).astype(jnp.bfloat16)
        if n == 0:
            for copy in weight_copies[1]:
                copy.start()
    done = [put(0, normed, outs[3])]
    later = [weight_copies[2], weight_copies[3], (copy_t, copy_w), (copy_m,)]
    for n in range(blocks):
        for copy in later[n]:
            copy.start()
        for copy in weight_copies[n]:
            copy.wait()
        cols = span(n)
        gate_pre = jnp.dot(normed[...], gate_v[:, cols], preferred_element_type=jnp.float32)
        up_pre = jnp.dot(normed[...], up_v[:, cols], preferred_element_type=jnp.float32)
        gate_pre = gate_pre * in_scale
        up_pre = up_pre * in_scale
        sig = jax.nn.sigmoid(gate_pre)
        activated = gate_pre * sig
        value = (activated * up_pre).astype(jnp.bfloat16)
        hidden[:, cols] = value
        hidden_t[cols] = value.T
        act[:, cols] = activated
        slope[:, cols] = up_pre * (sig * (1.0 + gate_pre * (1.0 - sig)))
        done.append(put(1 + 3 * n, hidden_t.at[cols], outs[0].at[cols]))
        done.append(put(2 + 3 * n, slope.at[:, cols], outs[1].at[:, cols]))
        done.append(put(3 + 3 * n, act.at[:, cols], outs[2].at[:, cols]))
    at_sem = 1 + 3 * blocks
    copy_w.wait()
    copy_t.wait()
    at = 0
    for n, size in enumerate(SIZES):
        cols = slice(at, at + size)
        theirs[:, cols] = jnp.dot(
            hidden[...], down_t[:, cols], preferred_element_type=jnp.float32
        ).astype(jnp.bfloat16)
        done.append(put(at_sem + 3 * n, theirs.at[:, cols], outs[4 + n]))
        at += size
    copy_m.wait()
    at = 0
    for n, size in enumerate(SIZES):
        cols = slice(at, at + size)
        at_tok = pl.multiple_of(core[0] * half + at, 128)
        offset[:, cols] = tok[:, pl.ds(at_tok, size)].astype(jnp.float32) - wanted[:, cols].astype(
            jnp.float32
        )
        done.append(put(at_sem + 3 * n + 2, offset.at[:, cols], outs[4 + 2 * count + n]))
        mine[:, cols] = jnp.dot(hidden[...], down_m[:, cols], preferred_element_type=jnp.float32)
        done.append(put(at_sem + 3 * n + 1, mine.at[:, cols], outs[4 + count + n]))
        at += size
    for copy in done:
        copy.wait()


def forward(core, tokens, targets, w_gate, w_up, w_down, in_scale):
    rows, width = tokens.shape
    count = w_gate.shape[1]
    half = width // 2
    anywhere = pl.BlockSpec(memory_space=pl.ANY)
    narrow = [jax.ShapeDtypeStruct((rows, size), jnp.bfloat16) for size in SIZES]
    wide = [jax.ShapeDtypeStruct((rows, size), jnp.float32) for size in SIZES]
    outs = [
        jax.ShapeDtypeStruct((count, rows), jnp.bfloat16),
        jax.ShapeDtypeStruct((rows, count), jnp.float32),
        jax.ShapeDtypeStruct((rows, count), jnp.float32),
        jax.ShapeDtypeStruct((rows, width), jnp.bfloat16),
        *narrow,
        *wide,
        *wide,
    ]
    blocks = count // BLOCK
    return pl.pallas_call(
        lambda *refs: forward_body(*refs, in_scale=in_scale),
        name="forward",
        in_specs=[pl.BlockSpec(memory_space=pltpu.SMEM)] + [anywhere] * 5,
        out_specs=[anywhere] * len(outs),
        out_shape=outs,
        scratch_shapes=[
            pltpu.VMEM((rows, width), jnp.bfloat16),
            pltpu.VMEM((width, count), jnp.bfloat16),
            pltpu.VMEM((width, count), jnp.bfloat16),
            pltpu.VMEM((count, half), jnp.bfloat16),
            pltpu.VMEM((count, half), jnp.bfloat16),
            pltpu.VMEM((rows, half), jnp.bfloat16),
            pltpu.VMEM((rows, count), jnp.bfloat16),
            pltpu.VMEM((count, rows), jnp.bfloat16),
            pltpu.VMEM((rows, count), jnp.float32),
            pltpu.VMEM((rows, count), jnp.float32),
            pltpu.VMEM((rows, width), jnp.bfloat16),
            pltpu.VMEM((rows, half), jnp.bfloat16),
            pltpu.VMEM((rows, half), jnp.float32),
            pltpu.VMEM((rows, half), jnp.float32),
            pltpu.SemaphoreType.DMA((2 + 2 * blocks + 3,)),
            pltpu.SemaphoreType.DMA((1 + 3 * blocks + 3 * len(SIZES),)),
        ],
        compiler_params=pltpu.CompilerParams(vmem_limit_bytes=58 * MIB),
    )(core[None].astype(jnp.int32), tokens, targets, w_gate, w_up, w_down)


def compute(tokens, targets, gate_weight, up_weight, down_weight):
    inputs = tokens[0]
    wanted = targets[0]
    w_gate = gate_weight[0]
    w_up = up_weight[0]
    w_down = down_weight[0]
    tok_count, width = inputs.shape
    mp_count = lax.axis_size("mp")
    hidden_all = w_gate.shape[1] * mp_count
    in_scale = 1.0 / width**0.5
    mid_scale = 1.0 / hidden_all**0.5
    step_size = hidden_all / 4.0
    half = width // 2
    core = lax.axis_index("mp") % 2
    mine = core * half
    theirs = half - mine

    outs = forward(core, inputs, wanted, w_gate, w_up, w_down, in_scale)
    hidden_t, slope_gate, act, normed = outs[:4]
    count = len(SIZES)
    sums_theirs, sums_mine, offsets = (outs[4 + n * count : 4 + (n + 1) * count] for n in range(3))

    def columns(array, start, size):
        return lax.dynamic_slice_in_dim(array, start, size, 1)

    def stepped_down(err, start):
        grad = dot(hidden_t, err, ((1,), (0,))) * mid_scale
        w_piece = columns(w_down, start, err.shape[1])
        new = (w_piece.astype(jnp.float32) - step_size * grad).astype(jnp.bfloat16)
        down_parts.append((start, both_ways(new)))

    totals = []
    far = []
    for n in range(count):
        arrived = other_core(sums_theirs[n])
        total = sums_mine[n] + arrived.astype(jnp.float32)
        rounded = total.astype(jnp.bfloat16)
        totals.append(total)
        far.append(other_chip(rounded))

    err_mine = []
    err_theirs = []
    down_parts = []
    at = 0
    for n, size in enumerate(SIZES):
        output = (totals[n] + far[n].astype(jnp.float32)) * mid_scale
        err = ((offsets[n] + output) / tok_count).astype(jnp.bfloat16)
        err_mine.append(err)
        err_theirs.append(other_core(err))
        stepped_down(err, mine + at)
        at += size
        if n == 1:
            first = jnp.concatenate(err_theirs, 1)
            stepped_down(first, theirs)
    stepped_down(err_theirs[2], theirs + SIZES[0] + SIZES[1])

    err_m = jnp.concatenate(err_mine, 1)
    err_t = jnp.concatenate([first, err_theirs[2]], 1)
    grad_hidden = (
        dot(err_m, columns(w_down, mine, half), ((1,), (1,)))
        + dot(err_t, columns(w_down, theirs, half), ((1,), (1,)))
    ) * mid_scale
    grad_gate = (grad_hidden * slope_gate).astype(jnp.bfloat16)
    grad_up = (grad_hidden * act).astype(jnp.bfloat16)

    def stepped(weight, grad_in, row, rows):
        grad_w = dot(normed[:, row : row + rows], grad_in, ((0,), (0,))) * in_scale
        new = (weight[row : row + rows].astype(jnp.float32) - step_size * grad_w).astype(
            jnp.bfloat16
        )
        return both_ways(new)

    gate_parts = stepped(w_gate, grad_gate, 0, width)
    up_parts = []
    row = 0
    for rows in UP_ROWS:
        up_parts.append((row, stepped(w_up, grad_up, row, rows)))
        row += rows

    down_out = jnp.zeros_like(w_down)
    for start, parts in down_parts:
        down_out = lax.dynamic_update_slice(down_out, mix_three(*parts), (0, start))
    gate_out = mix_rows(None, width, 0, gate_parts)
    up_out = gate_out[:16]
    for start, parts in up_parts:
        up_out = mix_rows(up_out, width, start, parts)
    return gate_out[None], up_out[None], down_out[None]


def solution(mesh):
    placed = (
        P("gossip", None, None),
        P("gossip", None, None),
        P("gossip", None, "mp"),
        P("gossip", None, "mp"),
        P("gossip", "mp", None),
    )
    return jax.shard_map(
        compute,
        mesh=mesh,
        in_specs=placed,
        out_specs=(P("gossip", None, "mp"), P("gossip", None, "mp"), P("gossip", "mp", None)),
        check_vma=False,
    )
```

```python
import jax
import jax.numpy as jnp
from jax import lax
from jax.experimental import pallas as pl
from jax.experimental.pallas import tpu as pltpu
from jax.sharding import PartitionSpec as P


SIZES = (256, 640, 128)
UP_ROWS = (1536, 256, 128, 128)
BLOCK = 256
MIB = 1024 * 1024


def exchange(value, parity):
    count = lax.axis_size("gossip")
    pairs = [(s, (s + 1 if s % 2 == parity else s - 1) % count) for s in range(count)]
    return lax.ppermute(value, "gossip", pairs)


def other_core(value):
    count = lax.axis_size("mp")
    return lax.ppermute(value, "mp", [(s, s ^ 1) for s in range(count)])


def other_chip(value):
    count = lax.axis_size("mp")
    return lax.ppermute(value, "mp", [(s, s ^ 2) for s in range(count)])


def both_ways(value):
    first = exchange(value, 1)
    second = exchange(value, 0)
    return first, value, second


def mix_three(lower, own, upper):
    total = lower.astype(jnp.float32) + own.astype(jnp.float32) + upper.astype(jnp.float32)
    return (total / 3.0).astype(jnp.bfloat16)


def mix_rows(before, rows_out, start, parts):
    rows, width = parts[1].shape
    block = min(rows, 256)

    def body(lower, own, upper, *rest):
        rest[-1][...] = mix_three(lower[...], own[...], upper[...])

    piece = pl.BlockSpec((block, width), lambda n: (n, 0))
    extra = [] if before is None else [before]
    return pl.pallas_call(
        body,
        grid=(rows // block,),
        in_specs=[piece] * 3 + [pl.BlockSpec(memory_space=pl.ANY)] * len(extra),
        out_specs=pl.BlockSpec((block, width), lambda n: (start // block + n, 0)),
        out_shape=jax.ShapeDtypeStruct((rows_out, width), jnp.bfloat16),
        input_output_aliases={3: 0} if start else {},
        compiler_params=pltpu.CompilerParams(vmem_limit_bytes=(56 if rows > 256 else 4) * MIB),
    )(*parts, *extra)


def dot(a, b, dims):
    return lax.dot_general(a, b, (dims, ((), ())), preferred_element_type=jnp.float32)


def forward_body(core, *refs, in_scale):
    tokens, w_gate, w_up, w_down = refs[:4]
    outs = refs[4 : 8 + len(SIZES)]
    (
        tok, gate_v, up_v, down_t, hidden, hidden_t, slope, act, theirs, in_sems, out_sems,
    ) = refs[8 + len(SIZES) :]
    _, width = tok.shape
    half = width // 2
    blocks = hidden.shape[1] // BLOCK
    at_theirs = pl.multiple_of((1 - core[0]) * half, half)
    done = []

    def fetch(n, src, dst):
        return pltpu.make_async_copy(src, dst, in_sems.at[n])

    def put(src, dst):
        copy = pltpu.make_async_copy(src, dst, out_sems.at[len(done)])
        copy.start()
        done.append(copy)

    def span(n):
        return slice(n * BLOCK, (n + 1) * BLOCK)

    tok_copy = fetch(0, tokens, tok)
    weight_copies = [
        (
            fetch(1 + 2 * n, w_gate.at[:, span(n)], gate_v.at[:, span(n)]),
            fetch(2 + 2 * n, w_up.at[:, span(n)], up_v.at[:, span(n)]),
        )
        for n in range(blocks)
    ]
    copy_t = fetch(1 + 2 * blocks, w_down.at[:, pl.ds(at_theirs, half)], down_t)
    for copy in (tok_copy, *weight_copies[0]):
        copy.start()
    tok_copy.wait()
    for copy in weight_copies[1]:
        copy.start()
    for n in range(blocks):
        if n + 2 < blocks:
            for copy in weight_copies[n + 2]:
                copy.start()
        elif n + 2 == blocks:
            copy_t.start()
        for copy in weight_copies[n]:
            copy.wait()
        if n == 0:
            wide = tok[...].astype(jnp.float32)
            scale = lax.rsqrt(jnp.mean(wide * wide, axis=-1, keepdims=True) + 1e-06)
        cols = span(n)
        gate_pre = jnp.dot(tok[...], gate_v[:, cols], preferred_element_type=jnp.float32)
        up_pre = jnp.dot(tok[...], up_v[:, cols], preferred_element_type=jnp.float32)
        gate_pre = gate_pre * (scale * in_scale)
        up_pre = up_pre * (scale * in_scale)
        sig = jax.nn.sigmoid(gate_pre)
        activated = gate_pre * sig
        value = (activated * up_pre).astype(jnp.bfloat16)
        hidden[:, cols] = value
        hidden_t[cols] = value.T
        act[:, cols] = (activated * scale).astype(jnp.bfloat16)
        slope[:, cols] = (up_pre * (sig * (1.0 + gate_pre * (1.0 - sig))) * scale).astype(
            jnp.bfloat16
        )
        put(hidden.at[:, cols], outs[0].at[:, cols])
        put(hidden_t.at[cols], outs[1].at[cols])
        put(slope.at[:, cols], outs[2].at[:, cols])
        put(act.at[:, cols], outs[3].at[:, cols])
    copy_t.wait()
    at = 0
    for n, size in enumerate(SIZES):
        cols = slice(at, at + size)
        theirs[:, cols] = jnp.dot(
            hidden[...], down_t[:, cols], preferred_element_type=jnp.float32
        ).astype(jnp.bfloat16)
        put(theirs.at[:, cols], outs[4 + n])
        at += size
    for copy in done:
        copy.wait()


def forward(core, tokens, w_gate, w_up, w_down, in_scale):
    rows, width = tokens.shape
    count = w_gate.shape[1]
    half = width // 2
    anywhere = pl.BlockSpec(memory_space=pl.ANY)
    shapes = [(rows, count), (count, rows), (rows, count), (rows, count)]
    outs = [
        jax.ShapeDtypeStruct(shape, jnp.bfloat16)
        for shape in shapes + [(rows, size) for size in SIZES]
    ]
    blocks = count // BLOCK
    return pl.pallas_call(
        lambda *refs: forward_body(*refs, in_scale=in_scale),
        name="forward",
        in_specs=[pl.BlockSpec(memory_space=pltpu.SMEM)] + [anywhere] * 4,
        out_specs=[anywhere] * len(outs),
        out_shape=outs,
        scratch_shapes=[
            pltpu.VMEM((rows, width), jnp.bfloat16),
            pltpu.VMEM((width, count), jnp.bfloat16),
            pltpu.VMEM((width, count), jnp.bfloat16),
            pltpu.VMEM((count, half), jnp.bfloat16),
            *[pltpu.VMEM(shape, jnp.bfloat16) for shape in shapes],
            pltpu.VMEM((rows, half), jnp.bfloat16),
            pltpu.SemaphoreType.DMA((2 + 2 * blocks,)),
            pltpu.SemaphoreType.DMA((4 * blocks + len(SIZES),)),
        ],
        compiler_params=pltpu.CompilerParams(vmem_limit_bytes=58 * MIB),
    )(core[None].astype(jnp.int32), tokens, w_gate, w_up, w_down)


def compute(tokens, targets, gate_weight, up_weight, down_weight):
    inputs = tokens[0]
    wanted = targets[0]
    w_gate = gate_weight[0]
    w_up = up_weight[0]
    w_down = down_weight[0]
    tok_count, width = inputs.shape
    mp_count = lax.axis_size("mp")
    hidden_all = w_gate.shape[1] * mp_count
    in_scale = 1.0 / width**0.5
    mid_scale = 1.0 / hidden_all**0.5
    step_size = hidden_all / 4.0
    half = width // 2
    core = lax.axis_index("mp") % 2
    mine = core * half
    theirs = half - mine

    outs = forward(core, inputs, w_gate, w_up, w_down, in_scale)
    hidden, hidden_t, slope_gate, act = outs[:4]
    sums_theirs = outs[4:]

    def columns(array, start, size):
        return lax.dynamic_slice_in_dim(array, start, size, 1)

    def stepped_down(err, start):
        grad = dot(hidden_t, err, ((1,), (0,))) * mid_scale
        w_piece = columns(w_down, start, err.shape[1])
        new = (w_piece.astype(jnp.float32) - step_size * grad).astype(jnp.bfloat16)
        down_parts.append((start, both_ways(new)))

    totals = []
    far = []
    at = 0
    for n, size in enumerate(SIZES):
        arrived = other_core(sums_theirs[n])
        own = dot(hidden, columns(w_down, mine + at, size), ((1,), (0,)))
        own = lax.optimization_barrier(own)
        total = own + arrived.astype(jnp.float32)
        rounded = total.astype(jnp.bfloat16)
        totals.append(total)
        far.append(other_chip(rounded))
        at += size

    err_mine = []
    err_theirs = []
    down_parts = []
    at = 0
    for n, size in enumerate(SIZES):
        output = (totals[n] + far[n].astype(jnp.float32)) * mid_scale
        offset = columns(inputs, mine + at, size).astype(jnp.float32) - columns(
            wanted, mine + at, size
        ).astype(jnp.float32)
        err = ((offset + output) / tok_count).astype(jnp.bfloat16)
        err_mine.append(err)
        err_theirs.append(other_core(err))
        stepped_down(err, mine + at)
        at += size
    err_t = jnp.concatenate(err_theirs, 1)
    stepped_down(err_t, theirs)

    grad_hidden = dot(
        jnp.concatenate(err_mine, 1), columns(w_down, mine, half), ((1,), (1,))
    ) + dot(err_t, columns(w_down, theirs, half), ((1,), (1,)))
    grad_hidden = grad_hidden * mid_scale
    grad_gate = (grad_hidden * slope_gate.astype(jnp.float32)).astype(jnp.bfloat16)
    grad_up = (grad_hidden * act.astype(jnp.float32)).astype(jnp.bfloat16)

    def stepped(weight, grad_in, row, rows):
        grad_w = dot(inputs[:, row : row + rows], grad_in, ((0,), (0,))) * in_scale
        new = (weight[row : row + rows].astype(jnp.float32) - step_size * grad_w).astype(
            jnp.bfloat16
        )
        return both_ways(new)

    gate_parts = stepped(w_gate, grad_gate, 0, width)
    up_parts = []
    row = 0
    for rows in UP_ROWS:
        up_parts.append((row, stepped(w_up, grad_up, row, rows)))
        row += rows

    down_out = jnp.zeros_like(w_down)
    for start, parts in down_parts:
        down_out = lax.dynamic_update_slice(down_out, mix_three(*parts), (0, start))
    gate_out = mix_rows(None, width, 0, gate_parts)
    up_out = gate_out[:16]
    for start, parts in up_parts:
        up_out = mix_rows(up_out, width, start, parts)
    return gate_out[None], up_out[None], down_out[None]


def solution(mesh):
    placed = (
        P("gossip", None, None),
        P("gossip", None, None),
        P("gossip", None, "mp"),
        P("gossip", None, "mp"),
        P("gossip", "mp", None),
    )
    return jax.shard_map(
        compute,
        mesh=mesh,
        in_specs=placed,
        out_specs=(P("gossip", None, "mp"), P("gossip", None, "mp"), P("gossip", "mp", None)),
        check_vma=False,
    )
```

```python
import jax
import jax.numpy as jnp
from jax import lax
from jax.experimental import pallas as pl
from jax.experimental.pallas import tpu as pltpu
from jax.sharding import PartitionSpec as P


SIZES = (384, 512, 128)
UP_ROWS = (1536, 256, 128, 128)
BLOCK = 256
ROW = 4
DETOUR = 416
MIB = 1024 * 1024


def exchange(value, parity):
    count = lax.axis_size("gossip")
    pairs = [(s, (s + 1 if s % 2 == parity else s - 1) % count) for s in range(count)]
    return lax.ppermute(value, "gossip", pairs)


def other_core(value):
    count = lax.axis_size("mp")
    return lax.ppermute(value, "mp", [(s, s ^ 1) for s in range(count)])


def other_chip(value):
    count = lax.axis_size("mp")
    return lax.ppermute(value, "mp", [(s, s ^ 2) for s in range(count)])


def both_ways(value):
    first = exchange(value, 1)
    second = exchange(value, 0)
    return first, value, second


def over_cycle(value, moves):
    count = lax.axis_size("gossip")
    pairs = [
        (s, (s + moves[s % ROW]) % count) for s in range(count) if s % ROW in moves
    ]
    return lax.ppermute(value, "gossip", pairs)


def mix_three(*parts):
    total = sum(part.astype(jnp.float32) for part in parts)
    return (total / 3.0).astype(jnp.bfloat16)


def mix_rows(before, rows_out, start, parts):
    rows, width = parts[1].shape
    block = min(rows, 256)

    def body(lower, own, upper, *rest):
        rest[-1][...] = mix_three(lower[...], own[...], upper[...])

    piece = pl.BlockSpec((block, width), lambda n: (n, 0))
    aliased = before is not None and before.shape[0] == rows_out
    extra = [] if before is None else [before]
    return pl.pallas_call(
        body,
        grid=(rows // block,),
        in_specs=[piece] * 3 + [pl.BlockSpec(memory_space=pl.ANY)] * len(extra),
        out_specs=pl.BlockSpec((block, width), lambda n: (start // block + n, 0)),
        out_shape=jax.ShapeDtypeStruct((rows_out, width), jnp.bfloat16),
        input_output_aliases={3: 0} if start else {},
        compiler_params=pltpu.CompilerParams(vmem_limit_bytes=(56 if rows > 256 else 4) * MIB),
    )(*parts, *extra)


def dot(a, b, dims):
    return lax.dot_general(a, b, (dims, ((), ())), preferred_element_type=jnp.float32)


def row_scale(tok):
    wide = tok[...].astype(jnp.float32)
    return lax.rsqrt(jnp.mean(wide * wide, axis=-1, keepdims=True) + 1e-06)


def gate_and_up(tok, gate, up, scale):
    gate_pre = jnp.dot(tok[...], gate, preferred_element_type=jnp.float32) * scale
    up_pre = jnp.dot(tok[...], up, preferred_element_type=jnp.float32) * scale
    return gate_pre, jax.nn.sigmoid(gate_pre), up_pre


def forward_body(
    core, tokens, w_gate, w_up, w_down, hidden_out, *refs, in_scale
):
    theirs_out = refs[: len(SIZES)]
    tok, gate_v, up_v, down_t, hidden, theirs, in_sems, out_sems = refs[len(SIZES) :]
    width = tok.shape[1]
    blocks = gate_v.shape[1] // BLOCK
    done = []

    def fetch(n, src, dst):
        return pltpu.make_async_copy(src, dst, in_sems.at[n])

    def put(src, dst):
        copy = pltpu.make_async_copy(src, dst, out_sems.at[len(done)])
        copy.start()
        done.append(copy)

    def span(n):
        return slice(n * BLOCK, (n + 1) * BLOCK)

    tok_copy = fetch(0, tokens, tok)
    weight_copies = [
        (
            fetch(1 + 2 * n, w_gate.at[:, span(n)], gate_v.at[:, span(n)]),
            fetch(2 + 2 * n, w_up.at[:, span(n)], up_v.at[:, span(n)]),
        )
        for n in range(blocks)
    ]
    at_theirs = pl.multiple_of((1 - core[0]) * (width // 2), width // 2)
    down_part = w_down.at[:, pl.ds(at_theirs, down_t.shape[1])]
    copy_t = fetch(1 + 2 * blocks, down_part, down_t)
    for copy in (tok_copy, *weight_copies[0]):
        copy.start()
    tok_copy.wait()
    for copy in weight_copies[1]:
        copy.start()
    for n in range(blocks):
        if n + 2 < blocks:
            for copy in weight_copies[n + 2]:
                copy.start()
        elif n + 2 == blocks:
            copy_t.start()
        for copy in weight_copies[n]:
            copy.wait()
        if n == 0:
            scale = row_scale(tok)
        cols = span(n)
        gate_pre, sig, up_pre = gate_and_up(tok, gate_v[:, cols], up_v[:, cols], scale * in_scale)
        hidden[:, cols] = (gate_pre * sig * up_pre).astype(jnp.bfloat16)
        put(hidden.at[:, cols], hidden_out.at[:, cols])
    copy_t.wait()
    at = 0
    for n, size in enumerate(SIZES):
        cols = slice(at, at + size)
        theirs[:, cols] = jnp.dot(
            hidden[...], down_t[:, cols], preferred_element_type=jnp.float32
        ).astype(jnp.bfloat16)
        put(theirs.at[:, cols], theirs_out[n])
        at += size
    for copy in done:
        copy.wait()


def forward(core, tokens, w_gate, w_up, w_down, in_scale):
    rows, width = tokens.shape
    count = w_gate.shape[1]
    anywhere = pl.BlockSpec(memory_space=pl.ANY)
    shapes = [(rows, count)] + [(rows, size) for size in SIZES]
    blocks = count // BLOCK
    return pl.pallas_call(
        lambda *refs: forward_body(*refs, in_scale=in_scale),
        name="forward",
        in_specs=[pl.BlockSpec(memory_space=pltpu.SMEM)] + [anywhere] * 4,
        out_specs=[anywhere] * len(shapes),
        out_shape=[jax.ShapeDtypeStruct(shape, jnp.bfloat16) for shape in shapes],
        scratch_shapes=[
            pltpu.VMEM((rows, width), jnp.bfloat16),
            pltpu.VMEM((width, count), jnp.bfloat16),
            pltpu.VMEM((width, count), jnp.bfloat16),
            pltpu.VMEM((count, width // 2), jnp.bfloat16),
            pltpu.VMEM((rows, count), jnp.bfloat16),
            pltpu.VMEM((rows, width // 2), jnp.bfloat16),
            pltpu.SemaphoreType.DMA((2 + 2 * blocks,)),
            pltpu.SemaphoreType.DMA((len(SIZES) + blocks,)),
        ],
        compiler_params=pltpu.CompilerParams(vmem_limit_bytes=58 * MIB),
    )(core[None].astype(jnp.int32), tokens, w_gate, w_up, w_down)


def slopes(tokens, w_gate, w_up, in_scale):
    rows, width = tokens.shape
    count = w_gate.shape[1]

    def body(tok, w_gate, w_up, slope, act):
        scale = row_scale(tok)
        gate_pre, sig, up_pre = gate_and_up(tok, w_gate[...], w_up[...], scale * in_scale)
        act[...] = (gate_pre * sig * scale).astype(jnp.bfloat16)
        slope[...] = (up_pre * (sig * (1.0 + gate_pre * (1.0 - sig))) * scale).astype(jnp.bfloat16)

    weights = pl.BlockSpec((width, BLOCK), lambda n: (0, n))
    across = pl.BlockSpec((rows, BLOCK), lambda n: (0, n))
    return pl.pallas_call(
        body,
        name="slopes",
        grid=(count // BLOCK,),
        in_specs=[pl.BlockSpec((rows, width), lambda n: (0, 0)), weights, weights],
        out_specs=[across, across],
        out_shape=[jax.ShapeDtypeStruct((rows, count), jnp.bfloat16)] * 2,
        compiler_params=pltpu.CompilerParams(vmem_limit_bytes=40 * MIB),
    )(tokens, w_gate, w_up)


def turned(value):
    rows, width = value.shape

    def body(value, out):
        out[...] = value[...].T

    return pl.pallas_call(
        body,
        name="turned",
        grid=(width // BLOCK,),
        in_specs=[pl.BlockSpec((rows, BLOCK), lambda n: (0, n))],
        out_specs=pl.BlockSpec((BLOCK, rows), lambda n: (n, 0)),
        out_shape=jax.ShapeDtypeStruct((width, rows), value.dtype),
        compiler_params=pltpu.CompilerParams(vmem_limit_bytes=4 * MIB),
    )(value)


def compute(tokens, targets, gate_weight, up_weight, down_weight):
    inputs = tokens[0]
    wanted = targets[0]
    w_gate = gate_weight[0]
    w_up = up_weight[0]
    w_down = down_weight[0]
    tok_count, width = inputs.shape
    mp_count = lax.axis_size("mp")
    hidden_all = w_gate.shape[1] * mp_count
    in_scale = 1.0 / width**0.5
    mid_scale = 1.0 / hidden_all**0.5
    step_size = hidden_all / 4.0
    half = width // 2
    core = lax.axis_index("mp") % 2
    mine = core * half
    theirs = half - mine

    hidden, *sums_theirs = forward(core, inputs, w_gate, w_up, w_down, in_scale)
    slope_gate, act = slopes(inputs, w_gate, w_up, in_scale)
    hidden_t = turned(hidden)

    def columns(array, start, size):
        return lax.dynamic_slice_in_dim(array, start, size, 1)

    def stepped_down(err, start):
        grad = dot(hidden_t, err, ((1,), (0,))) * mid_scale
        w_piece = columns(w_down, start, err.shape[1])
        return (w_piece.astype(jnp.float32) - step_size * grad).astype(jnp.bfloat16)

    def send_down(err, start):
        down_parts.append((start, both_ways(stepped_down(err, start))))

    totals = []
    far = []
    at = 0
    for n, size in enumerate(SIZES):
        arrived = other_core(sums_theirs[n])
        own = dot(hidden, columns(w_down, mine + at, size), ((1,), (0,)))
        own = lax.optimization_barrier(own)
        total = own + arrived.astype(jnp.float32)
        rounded = total.astype(jnp.bfloat16)
        totals.append(total)
        far.append(other_chip(rounded))
        at += size

    err_mine = []
    err_theirs = []
    down_parts = []
    at = 0
    for n, size in enumerate(SIZES):
        output = (totals[n] + far[n].astype(jnp.float32)) * mid_scale
        offset = columns(inputs, mine + at, size).astype(jnp.float32) - columns(
            wanted, mine + at, size
        ).astype(jnp.float32)
        err = ((offset + output) / tok_count).astype(jnp.bfloat16)
        err_mine.append(err)
        err_theirs.append(other_core(err))
        if n:
            send_down(err, mine + at)
        else:
            new = stepped_down(err, mine)
            even = exchange(new, 0)
            inside = over_cycle(new, {1: 1, 2: -1})
            relay = over_cycle(new[:DETOUR], {3: -1, 0: 1})
            crossed = over_cycle(new[DETOUR:], {3: 1, 0: -1})
            relay = over_cycle(relay, {2: ROW, 1: -ROW})
            relay = over_cycle(relay, {2: -1, 1: 1})
            relay = over_cycle(relay, {1: -1, 2: 1})
            down_parts.append((mine, (new, even, inside, (relay, crossed))))
        at += size
    err_t = jnp.concatenate(err_theirs, 1)
    send_down(err_t, theirs)

    grad_hidden = dot(
        jnp.concatenate(err_mine, 1), columns(w_down, mine, half), ((1,), (1,))
    ) + dot(err_t, columns(w_down, theirs, half), ((1,), (1,)))
    grad_hidden = grad_hidden * mid_scale
    grad_gate = (grad_hidden * slope_gate.astype(jnp.float32)).astype(jnp.bfloat16)
    grad_up = (grad_hidden * act.astype(jnp.float32)).astype(jnp.bfloat16)

    def stepped(weight, grad_in, row, rows):
        grad_w = dot(inputs[:, row : row + rows], grad_in, ((0,), (0,))) * in_scale
        new = (weight[row : row + rows].astype(jnp.float32) - step_size * grad_w).astype(
            jnp.bfloat16
        )
        return both_ways(new)

    gate_parts = stepped(w_gate, grad_gate, 0, width)
    up_parts = []
    row = 0
    for rows in UP_ROWS:
        up_parts.append((row, stepped(w_up, grad_up, row, rows)))
        row += rows

    down_out = jnp.zeros_like(w_down)
    for n, (start, parts) in enumerate(down_parts):
        if n == 0:
            row = 0
            for part in parts[3]:
                rows = slice(row, row + part.shape[0])
                mixed = mix_three(*(whole[rows] for whole in parts[:3]), part)
                down_out = lax.dynamic_update_slice(down_out, mixed, (row, start))
                row += part.shape[0]
        else:
            down_out = lax.dynamic_update_slice(down_out, mix_three(*parts), (0, start))
    gate_out = mix_rows(None, width, 0, gate_parts)
    up_out = gate_out[:16]
    for start, parts in up_parts:
        up_out = mix_rows(up_out, width, start, parts)
    return gate_out[None], up_out[None], down_out[None]


def solution(mesh):
    placed = (
        P("gossip", None, None),
        P("gossip", None, None),
        P("gossip", None, "mp"),
        P("gossip", None, "mp"),
        P("gossip", "mp", None),
    )
    return jax.shard_map(
        compute,
        mesh=mesh,
        in_specs=placed,
        out_specs=(P("gossip", None, "mp"), P("gossip", None, "mp"), P("gossip", "mp", None)),
        check_vma=False,
    )
```

```python
import jax
import jax.numpy as jnp
from jax import lax
from jax.experimental import pallas as pl
from jax.experimental.pallas import tpu as pltpu
from jax.sharding import PartitionSpec as P


SIZES = (384, 512, 128)
UP_ROWS = (1792, 128, 64, 64)
BLOCK = 256
ROW = 4
DETOUR = 400
MIB = 1024 * 1024


def exchange(value, parity):
    count = lax.axis_size("gossip")
    pairs = [(s, (s + 1 if s % 2 == parity else s - 1) % count) for s in range(count)]
    return lax.ppermute(value, "gossip", pairs)


def other_core(value):
    count = lax.axis_size("mp")
    return lax.ppermute(value, "mp", [(s, s ^ 1) for s in range(count)])


def other_chip(value):
    count = lax.axis_size("mp")
    return lax.ppermute(value, "mp", [(s, s ^ 2) for s in range(count)])


def both_ways(value):
    first = exchange(value, 1)
    second = exchange(value, 0)
    return first, value, second


def over_cycle(value, moves):
    count = lax.axis_size("gossip")
    pairs = [
        (s, (s + moves[s % ROW]) % count) for s in range(count) if s % ROW in moves
    ]
    return lax.ppermute(value, "gossip", pairs)


def mix_three(*parts):
    total = sum(part.astype(jnp.float32) for part in parts)
    return (total / 3.0).astype(jnp.bfloat16)


def mix_rows(before, rows_out, start, parts):
    rows, width = parts[1].shape
    block = min(rows, 256)

    def body(lower, own, upper, *rest):
        rest[-1][...] = mix_three(lower[...], own[...], upper[...])

    piece = pl.BlockSpec((block, width), lambda n: (n, 0))
    aliased = before is not None and before.shape[0] == rows_out
    extra = [] if before is None else [before]
    return pl.pallas_call(
        body,
        grid=(rows // block,),
        in_specs=[piece] * 3 + [pl.BlockSpec(memory_space=pl.ANY)] * len(extra),
        out_specs=pl.BlockSpec((block, width), lambda n: (start // block + n, 0)),
        out_shape=jax.ShapeDtypeStruct((rows_out, width), jnp.bfloat16),
        input_output_aliases={3: 0} if start else {},
        compiler_params=pltpu.CompilerParams(vmem_limit_bytes=(56 if rows > 256 else 4) * MIB),
    )(*parts, *extra)


def dot(a, b, dims):
    return lax.dot_general(a, b, (dims, ((), ())), preferred_element_type=jnp.float32)


def row_scale(tok):
    wide = tok[...].astype(jnp.float32)
    return lax.rsqrt(jnp.mean(wide * wide, axis=-1, keepdims=True) + 1e-06)


def gate_and_up(tok, gate, up, scale):
    gate_pre = jnp.dot(tok[...], gate, preferred_element_type=jnp.float32) * scale
    up_pre = jnp.dot(tok[...], up, preferred_element_type=jnp.float32) * scale
    return gate_pre, jax.nn.sigmoid(gate_pre), up_pre


def forward_body(
    core, tokens, w_gate, w_up, w_down, hidden_out, theirs_out,
    tok, gate_v, up_v, down_t, hidden, theirs, in_sems, out_sems, *, in_scale
):
    width = tok.shape[1]
    blocks = gate_v.shape[1] // BLOCK
    done = []

    def fetch(n, src, dst):
        return pltpu.make_async_copy(src, dst, in_sems.at[n])

    def put(src, dst):
        copy = pltpu.make_async_copy(src, dst, out_sems.at[len(done)])
        copy.start()
        done.append(copy)

    def span(n):
        return slice(n * BLOCK, (n + 1) * BLOCK)

    tok_copy = fetch(0, tokens, tok)
    weight_copies = [
        (
            fetch(1 + 2 * n, w_gate.at[:, span(n)], gate_v.at[:, span(n)]),
            fetch(2 + 2 * n, w_up.at[:, span(n)], up_v.at[:, span(n)]),
        )
        for n in range(blocks)
    ]
    at_theirs = pl.multiple_of((1 - core[0]) * (width // 2), width // 2)
    down_part = w_down.at[:, pl.ds(at_theirs, down_t.shape[1])]
    copy_t = fetch(1 + 2 * blocks, down_part, down_t)
    for copy in (tok_copy, *weight_copies[0]):
        copy.start()
    tok_copy.wait()
    for copy in weight_copies[1]:
        copy.start()
    for n in range(blocks):
        if n + 2 < blocks:
            for copy in weight_copies[n + 2]:
                copy.start()
        elif n + 2 == blocks:
            copy_t.start()
        for copy in weight_copies[n]:
            copy.wait()
        if n == 0:
            scale = row_scale(tok)
        cols = span(n)
        gate_pre, sig, up_pre = gate_and_up(tok, gate_v[:, cols], up_v[:, cols], scale * in_scale)
        hidden[:, cols] = (gate_pre * sig * up_pre).astype(jnp.bfloat16)
        put(hidden.at[:, cols], hidden_out.at[:, cols])
    copy_t.wait()
    theirs[...] = jnp.dot(hidden[...], down_t[...], preferred_element_type=jnp.float32).astype(
        jnp.bfloat16
    )
    put(theirs, theirs_out)
    for copy in done:
        copy.wait()


def forward(core, tokens, w_gate, w_up, w_down, in_scale):
    rows, width = tokens.shape
    count = w_gate.shape[1]
    anywhere = pl.BlockSpec(memory_space=pl.ANY)
    shapes = [(rows, count), (rows, SIZES[0])]
    blocks = count // BLOCK
    return pl.pallas_call(
        lambda *refs: forward_body(*refs, in_scale=in_scale),
        name="forward",
        in_specs=[pl.BlockSpec(memory_space=pltpu.SMEM)] + [anywhere] * 4,
        out_specs=[anywhere] * len(shapes),
        out_shape=[jax.ShapeDtypeStruct(shape, jnp.bfloat16) for shape in shapes],
        scratch_shapes=[
            pltpu.VMEM((rows, width), jnp.bfloat16),
            pltpu.VMEM((width, count), jnp.bfloat16),
            pltpu.VMEM((width, count), jnp.bfloat16),
            pltpu.VMEM((count, SIZES[0]), jnp.bfloat16),
            *[pltpu.VMEM(shape, jnp.bfloat16) for shape in shapes],
            pltpu.SemaphoreType.DMA((2 + 2 * blocks,)),
            pltpu.SemaphoreType.DMA((1 + blocks,)),
        ],
        compiler_params=pltpu.CompilerParams(vmem_limit_bytes=58 * MIB),
    )(core[None].astype(jnp.int32), tokens, w_gate, w_up, w_down)


def slopes(tokens, w_gate, w_up, in_scale):
    rows, width = tokens.shape
    count = w_gate.shape[1]

    def body(tok, w_gate, w_up, slope, act):
        scale = row_scale(tok)
        gate_pre, sig, up_pre = gate_and_up(tok, w_gate[...], w_up[...], scale * in_scale)
        act[...] = (gate_pre * sig * scale).astype(jnp.bfloat16)
        slope[...] = (up_pre * (sig * (1.0 + gate_pre * (1.0 - sig))) * scale).astype(jnp.bfloat16)

    weights = pl.BlockSpec((width, BLOCK), lambda n: (0, n))
    across = pl.BlockSpec((rows, BLOCK), lambda n: (0, n))
    return pl.pallas_call(
        body,
        name="slopes",
        grid=(count // BLOCK,),
        in_specs=[pl.BlockSpec((rows, width), lambda n: (0, 0)), weights, weights],
        out_specs=[across, across],
        out_shape=[jax.ShapeDtypeStruct((rows, count), jnp.bfloat16)] * 2,
        compiler_params=pltpu.CompilerParams(vmem_limit_bytes=40 * MIB),
    )(tokens, w_gate, w_up)


def turned(value):
    rows, width = value.shape

    def body(value, out):
        out[...] = value[...].T

    return pl.pallas_call(
        body,
        name="turned",
        grid=(width // BLOCK,),
        in_specs=[pl.BlockSpec((rows, BLOCK), lambda n: (0, n))],
        out_specs=pl.BlockSpec((BLOCK, rows), lambda n: (n, 0)),
        out_shape=jax.ShapeDtypeStruct((width, rows), value.dtype),
        compiler_params=pltpu.CompilerParams(vmem_limit_bytes=4 * MIB),
    )(value)


def compute(tokens, targets, gate_weight, up_weight, down_weight):
    inputs = tokens[0]
    wanted = targets[0]
    w_gate = gate_weight[0]
    w_up = up_weight[0]
    w_down = down_weight[0]
    tok_count, width = inputs.shape
    mp_count = lax.axis_size("mp")
    hidden_all = w_gate.shape[1] * mp_count
    in_scale = 1.0 / width**0.5
    mid_scale = 1.0 / hidden_all**0.5
    step_size = hidden_all / 4.0
    half = width // 2
    core = lax.axis_index("mp") % 2
    mine = core * half
    theirs = half - mine

    hidden, first_sent = forward(core, inputs, w_gate, w_up, w_down, in_scale)
    slope_gate, act = slopes(inputs, w_gate, w_up, in_scale)
    hidden_t = turned(hidden)

    def columns(array, start, size):
        return lax.dynamic_slice_in_dim(array, start, size, 1)

    def stepped_down(err, start):
        grad = dot(hidden_t, err, ((1,), (0,))) * mid_scale
        w_piece = columns(w_down, start, err.shape[1])
        return (w_piece.astype(jnp.float32) - step_size * grad).astype(jnp.bfloat16)

    def send_down(err, start):
        down_parts.append((start, both_ways(stepped_down(err, start))))

    rest = half - SIZES[0]
    rest_sent = dot(hidden, columns(w_down, theirs + SIZES[0], rest), ((1,), (0,)))
    rest_sent = rest_sent.astype(jnp.bfloat16)
    arrived = []
    own = []
    for sent, start, size in ((first_sent, 0, SIZES[0]), (rest_sent, SIZES[0], rest)):
        arrived.append(other_core(sent))
        value = dot(hidden, columns(w_down, mine + start, size), ((1,), (0,)))
        own.append(lax.optimization_barrier(value))
    totals = []
    far = []
    at = 0
    for n, size in enumerate(SIZES):
        which = min(n, 1)
        cols = slice(at - which * SIZES[0], at - which * SIZES[0] + size)
        total = own[which][:, cols] + arrived[which][:, cols].astype(jnp.float32)
        rounded = total.astype(jnp.bfloat16)
        totals.append(total)
        far.append(other_chip(rounded))
        at += size

    err_mine = []
    err_theirs = []
    down_parts = []
    at = 0
    for n, size in enumerate(SIZES):
        output = (totals[n] + far[n].astype(jnp.float32)) * mid_scale
        offset = columns(inputs, mine + at, size).astype(jnp.float32) - columns(
            wanted, mine + at, size
        ).astype(jnp.float32)
        err = ((offset + output) / tok_count).astype(jnp.bfloat16)
        err_mine.append(err)
        err_theirs.append(other_core(err))
        if n:
            send_down(err, mine + at)
        else:
            new = stepped_down(err, mine)
            even = exchange(new, 0)
            inside = over_cycle(new, {1: 1, 2: -1})
            relay, crossed = lax.optimization_barrier((new[:DETOUR], new[DETOUR:]))
            relay = over_cycle(relay, {3: -1, 0: 1})
            crossed = over_cycle(crossed, {3: 1, 0: -1})
            relay = over_cycle(relay, {2: ROW, 1: -ROW})
            relay = over_cycle(relay, {2: -1, 1: 1})
            relay = over_cycle(relay, {1: -1, 2: 1})
            down_parts.append((mine, (new, even, inside, (relay, crossed))))
        at += size
    err_t = jnp.concatenate(err_theirs, 1)
    send_down(err_t, theirs)

    grad_hidden = dot(
        jnp.concatenate(err_mine, 1), columns(w_down, mine, half), ((1,), (1,))
    ) + dot(err_t, columns(w_down, theirs, half), ((1,), (1,)))
    grad_hidden = grad_hidden * mid_scale
    grad_gate = (grad_hidden * slope_gate.astype(jnp.float32)).astype(jnp.bfloat16)
    grad_up = (grad_hidden * act.astype(jnp.float32)).astype(jnp.bfloat16)

    def stepped(weight, grad_in, row, rows):
        grad_w = dot(inputs[:, row : row + rows], grad_in, ((0,), (0,))) * in_scale
        new = (weight[row : row + rows].astype(jnp.float32) - step_size * grad_w).astype(
            jnp.bfloat16
        )
        return both_ways(new)

    gate_parts = stepped(w_gate, grad_gate, 0, width)
    up_parts = []
    row = 0
    for rows in UP_ROWS:
        up_parts.append((row, stepped(w_up, grad_up, row, rows)))
        row += rows

    down_out = jnp.zeros_like(w_down)
    for n, (start, parts) in enumerate(down_parts):
        if n == 0:
            row = 0
            for part in parts[3]:
                rows = slice(row, row + part.shape[0])
                mixed = mix_three(*(whole[rows] for whole in parts[:3]), part)
                down_out = lax.dynamic_update_slice(down_out, mixed, (row, start))
                row += part.shape[0]
        else:
            down_out = lax.dynamic_update_slice(down_out, mix_three(*parts), (0, start))
    gate_out = mix_rows(None, width, 0, gate_parts)
    up_out = gate_out[:16]
    for start, parts in up_parts:
        up_out = mix_rows(up_out, width, start, parts)
    return gate_out[None], up_out[None], down_out[None]


def solution(mesh):
    placed = (
        P("gossip", None, None),
        P("gossip", None, None),
        P("gossip", None, "mp"),
        P("gossip", None, "mp"),
        P("gossip", "mp", None),
    )
    return jax.shard_map(
        compute,
        mesh=mesh,
        in_specs=placed,
        out_specs=(P("gossip", None, "mp"), P("gossip", None, "mp"), P("gossip", "mp", None)),
        check_vma=False,
    )
```
